1024 devices in a mesh: role: 2 (over x_hi), ctx: 32 (over z, core), head: 16 (over x_lo, y).
Axes of the slice: x: 4 (x_hi: 2, x_lo: 2; x = x_hi * 2 + x_lo), y: 8, z: 16, core: 2. Of those that a mesh axis runs over, the one named last changes fastest.
Arguments:
- tokens: bfloat16 [2, 2048, 7168], P('role', 'ctx', 'head'), may hold values from -6 to 6
- latent_cache: bfloat16 [1536, 576], P('ctx'), may hold values from -400 to 400
- offset: int32 [1], replicated, may hold values from 385 to 1536
- bounds: int32 [2048], P('ctx'), may hold values from 1 to 3584
- query_down: bfloat16 [7168, 1536], P('head'), may hold values from -0.0625 to 0.0625
- latent_down_weight: bfloat16 [7168, 576], P('head'), may hold values from -0.0625 to 0.0625
- query_gain: float32 [1536], replicated, may hold values from 0.25 to 1.75
- latent_norm_gain: float32 [512], replicated, may hold values from 0.25 to 1.75
- query_up: bfloat16 [1536, 24576], P(None, 'head'), may hold values from -0.15625 to 0.15625
- key_up_transposed: bfloat16 [128, 128, 512], P('head'), may hold values from -0.5 to 0.5
- value_up_weight: bfloat16 [128, 512, 128], P('head'), may hold values from -0.25 to 0.25
Outputs:
- attended: bfloat16 [2, 2048, 16384], P('role', 'ctx', 'head')
The draws below stay inside these ranges and needn't reach their ends.
Inputs may be any that keep to these rules, and one draw needn't show every extreme that they name: `bounds`: A continuation row at position p sees keys at positions below p and itself. Cache slots from offset on are unused; the block's tokens sit at positions offset to offset + 2047.
All inputs are finite; a program needn't handle non-finite values.
Results may differ from the reference program's by a relative error of at most 0.02.
Values may be sent and summed in bfloat16 or wider, within the bound.
A program may use at most 64 MiB of HBM per device.

```python
import jax
import jax.numpy as jnp
from jax import lax

MODEL_WIDTH = 7168
QRANK = 1536
LATENT_WIDTH = 512
ROTARY_DIM = 64
PLAIN_QUERY_DIM = 128
VALUE_HEAD_SIZE = 128
ATTENTION_HEADS = 128
ROWS = 2048
CACHE_SLOTS = 1536


def draw_latent_cache(key, part):
    drawn_key_part, rotary_key = jax.random.split(jax.random.fold_in(key, 11), 2)
    value_rows = jnp.clip(jax.random.normal(drawn_key_part, (CACHE_SLOTS, LATENT_WIDTH + ROTARY_DIM), jnp.float32), -4.0, 4.0)
    strengths = (20.0, 45.0, 100.0)
    inserted_cache = (2, CACHE_SLOTS // 8, CACHE_SLOTS // 4)
    for element_count in range(3):
        rotation_sign = jnp.clip(jax.random.normal(jax.random.fold_in(rotary_key, element_count), (ROTARY_DIM,), jnp.float32), -3.0, 3.0)
        rotation_sign = rotation_sign * strengths[element_count]
        for second_half in range(2):
            value_rows = value_rows.at[inserted_cache[element_count] + second_half, LATENT_WIDTH:].set(rotation_sign)
    return value_rows.astype(jnp.bfloat16)


def plant(array, rng, least, high):
    place = [jax.random.randint(jax.random.fold_in(rng, axis), (), 0, length) for axis, length in enumerate(array.shape)]
    widest = array.shape.index(max(array.shape))
    next_to = place[:widest] + [(place[widest] + 1) % array.shape[widest]] + place[widest + 1:]
    return array.at[tuple(place)].set(least).at[tuple(next_to)].set(high)


def level_of(key, dims, cuts, smallest, largest):
    factor_of = 1.0
    for axis_at, blocks in cuts:
        heights = jax.random.uniform(jax.random.fold_in(jax.random.fold_in(key, 6), axis_at), (blocks,), jnp.float32, smallest / len(cuts), largest / len(cuts))
        factor_of = factor_of * jnp.repeat(jnp.exp(heights), dims[axis_at] // blocks).reshape((-1,) + (1,) * (len(dims) - 1 - axis_at))
    return factor_of


def scatter_about(stream_key, dims, scale, limit, pieces=(), kind=jnp.bfloat16):
    result = jax.random.normal(stream_key, dims, jnp.float32) * scale
    if len(pieces) > 0:
        result = level_of(stream_key, dims, pieces, -0.22, 0.18) * result
    return jnp.clip(result, min=-limit, max=limit).astype(kind)


def setup_inputs(seed: int = 0) -> dict:
    seeds = jax.random.split(jax.random.key(seed), 12)
    return {
        "tokens": scatter_about(seeds[0], (2, ROWS, MODEL_WIDTH), 1.0, 6.0, ((0, 2), (1, 32), (2, 16))),
        "latent_cache": draw_latent_cache(jax.random.fold_in(seeds[11], 71), 0),
        "offset": jax.random.randint(seeds[2], (1,), CACHE_SLOTS // 4 + 1, CACHE_SLOTS + 1).astype(jnp.int32),
        "bounds": plant(jax.random.randint(seeds[3], (ROWS,), 1, CACHE_SLOTS + ROWS + 1), jax.random.fold_in(seeds[3], 1), 1, CACHE_SLOTS + ROWS).astype(jnp.int32),
        "query_down": scatter_about(seeds[4], (MODEL_WIDTH, QRANK), MODEL_WIDTH ** -0.5, 0.0625, ((0, 16),)),
        "latent_down_weight": scatter_about(seeds[5], (MODEL_WIDTH, LATENT_WIDTH + ROTARY_DIM), MODEL_WIDTH ** -0.5, 0.0625, ((0, 16),)),
        "query_gain": jnp.clip(1.0 + 0.15 * jax.random.normal(seeds[6], (QRANK,), jnp.float32), 0.25, 1.75),
        "latent_norm_gain": jnp.clip(1.0 + 0.15 * jax.random.normal(seeds[7], (LATENT_WIDTH,), jnp.float32), 0.25, 1.75),
        "query_up": scatter_about(seeds[8], (QRANK, ATTENTION_HEADS * (PLAIN_QUERY_DIM + ROTARY_DIM)), QRANK ** -0.5, 0.15625, ((1, 16),)),
        "key_up_transposed": scatter_about(seeds[9], (ATTENTION_HEADS, PLAIN_QUERY_DIM, LATENT_WIDTH), PLAIN_QUERY_DIM ** -0.5, 0.5, ((0, 16),)),
        "value_up_weight": scatter_about(seeds[10], (ATTENTION_HEADS, LATENT_WIDTH, VALUE_HEAD_SIZE), LATENT_WIDTH ** -0.5, 0.25, ((0, 16),)),
    }


EPS = 1e-06

def root_mean_norm(value_rows, gain):
    return value_rows * lax.rsqrt(lax.optimization_barrier(jnp.mean(value_rows * value_rows, axis=-1, keepdims=True)) + EPS) * gain.astype(jnp.float32)

def apply_rotary(value_rows, token_positions):
    half = value_rows.shape[-1] // 2
    freqs = 10000.0 ** (-jnp.arange(half, dtype=jnp.float32) / half)
    angles = token_positions.astype(jnp.float32)[:, None] * freqs[None, :]
    if value_rows.ndim == 3:
        angles = angles[:, None, :]
    first = value_rows[..., :half]
    second_half = value_rows[..., half:]
    cosine = jnp.cos(angles)
    sine = jnp.sin(angles)
    return jnp.concatenate([first * cosine - second_half * sine, first * sine + second_half * cosine], axis=-1)

def project(inputs, token_positions, query_down, latent_down_weight, query_gain, latent_norm_gain, query_up, key_up_transposed):
    query_lat = jnp.dot(inputs, query_down, preferred_element_type=jnp.float32)
    key_value_latent = jnp.dot(inputs, latent_down_weight, preferred_element_type=jnp.float32)
    query_norm = root_mean_norm(query_lat, query_gain).astype(jnp.bfloat16)
    latent_vector = root_mean_norm(key_value_latent[:, :LATENT_WIDTH], latent_norm_gain)
    rotary_key_part = apply_rotary(key_value_latent[:, LATENT_WIDTH:], token_positions)
    self_key_row = jnp.concatenate([latent_vector, rotary_key_part], axis=-1).astype(jnp.bfloat16)
    queries = jnp.dot(query_norm, query_up, preferred_element_type=jnp.float32)
    queries = queries.reshape(queries.shape[0], ATTENTION_HEADS, PLAIN_QUERY_DIM + ROTARY_DIM)
    query_nope = queries[..., :PLAIN_QUERY_DIM].astype(jnp.bfloat16)
    query_rot = apply_rotary(queries[..., PLAIN_QUERY_DIM:], token_positions).astype(jnp.bfloat16)
    absorbed = jnp.einsum('rhn,hnc->rhc', query_nope.astype(jnp.float32), key_up_transposed.astype(jnp.float32)).astype(jnp.bfloat16)
    return (jnp.concatenate([absorbed, query_rot], axis=-1), self_key_row)

def attend(queries, self_key_row, limits, every_key_row, key_pos, key_valid, value_up_weight):
    softmax_scale = (PLAIN_QUERY_DIM + ROTARY_DIM) ** (-0.5)

    def one_head(operands):
        head_query, head_value = operands
        scores = jnp.dot(head_query, every_key_row.T, preferred_element_type=jnp.float32) * softmax_scale
        key_mask = key_valid[None, :] & (key_pos[None, :] < limits[:, None])
        self_score = lax.optimization_barrier(jnp.sum(head_query.astype(jnp.float32) * self_key_row.astype(jnp.float32), axis=-1)) * softmax_scale
        row_max = jnp.maximum(lax.optimization_barrier(jnp.max(jnp.where(key_mask, scores, -jnp.inf), axis=-1)), self_score)
        attention_weights = jnp.where(key_mask, jnp.exp(scores - row_max[:, None]), 0.0)
        self_attend_weight = jnp.exp(self_score - row_max)
        denom = lax.optimization_barrier(jnp.sum(attention_weights, axis=-1)) + self_attend_weight
        numerator_sum = jnp.dot(attention_weights.astype(jnp.bfloat16), every_key_row[:, :LATENT_WIDTH], preferred_element_type=jnp.float32)
        numerator_sum = numerator_sum + self_attend_weight.astype(jnp.bfloat16).astype(jnp.float32)[:, None] * self_key_row[:, :LATENT_WIDTH].astype(jnp.float32)
        out_latent = (numerator_sum / denom[:, None]).astype(jnp.bfloat16)
        return jnp.dot(out_latent, head_value, preferred_element_type=jnp.float32).astype(jnp.bfloat16)
    per_head = lax.map(one_head, (jnp.transpose(queries, (1, 0, 2)), value_up_weight))
    return jnp.transpose(per_head, (1, 0, 2)).reshape(queries.shape[0], ATTENTION_HEADS * VALUE_HEAD_SIZE)

def reference(tokens, latent_cache, offset, bounds, query_down, latent_down_weight, query_gain, latent_norm_gain, query_up, key_up_transposed, value_up_weight):
    block_start = offset[0]
    row_index = jnp.arange(ROWS, dtype=jnp.int32)
    block_pos = block_start + row_index
    weights_all = (query_down, latent_down_weight, query_gain, latent_norm_gain, query_up, key_up_transposed)
    block_query, block_key = project(tokens[0], block_pos, *weights_all)
    cont_query, cont_key = project(tokens[1], bounds, *weights_all)
    cache_pos = jnp.arange(CACHE_SLOTS, dtype=jnp.int32)
    every_key_row = jnp.concatenate([latent_cache, block_key], axis=0)
    key_pos = jnp.concatenate([cache_pos, block_pos], axis=0)
    key_valid = jnp.concatenate([cache_pos < block_start, jnp.ones((ROWS,), dtype=bool)], axis=0)
    block_out = attend(block_query, block_key, block_pos, every_key_row, key_pos, key_valid, value_up_weight)
    cont_out = attend(cont_query, cont_key, bounds, every_key_row, key_pos, key_valid, value_up_weight)
    return jnp.stack([block_out, cont_out], axis=0)
```

```python
import jax
import jax.numpy as jnp
import numpy as np
from jax import lax
from jax.experimental import pallas as pl
from jax.experimental.pallas import tpu as pltpu
from jax.sharding import PartitionSpec as P

LAT = 512
ROT = 64
KEY = LAT + ROT
NOPE = 128
VAL = 128
HEADS = 8
ROWS = 64
CROWS = 48
QRANK = 1536
QBLOCKS = QRANK // 128
ZS = 16
NCTX = 2 * ZS
NHEAD = 16
EPS = 1e-06
SCALE = (NOPE + ROT) ** (-0.5)
NEG = -1e30
MESH = pl.DeviceIdType.MESH
F32 = jnp.float32
BF16 = jnp.bfloat16
SUBS = 2
PIECE = ROWS // SUBS
QCOLS = HEADS * ROWS
scope = jax.named_scope


def remote(src, dst, send, recv, **where):
    return pltpu.make_async_remote_copy(
        src_ref=src, dst_ref=dst, send_sem=send, recv_sem=recv, device_id=where, device_id_type=MESH
    )


def swap_halves(v):
    return jnp.concatenate([v[:, ROT // 2 :], v[:, : ROT // 2]], axis=1)


def body(
    tokens, cache, query_down, latent_down, query_up, key_up,
    offset, bounds, freqs, query_gain, latent_gain,
    out,
    xv, ldv, qdv, qupv, kupv, cos, sin,
    stage_kv, stage_q, rs_kv, rs_q, qc, ks, kc, kb, qn, qs, m_ref, l_ref, acc,
    load_sem, rs_send, rs_recv, qag_send, qag_recv, kag_send, kag_recv,
    cz_send, cz_recv, cp_send, cp_recv, bz_send, bz_recv, bp_send, bp_recv,
    ready_z, ready_role,
):
    role = lax.axis_index("role")
    c = lax.axis_index("ctx")
    h = lax.axis_index("head")
    z, core = c // 2, c % 2
    up, down = (c + 2) % NCTX, (c + NCTX - 2) % NCTX
    partner = c + 1 - 2 * core
    group = h // 4
    is_kv = h % 4 == 3
    q_block = 3 * group + h % 4
    tail = []

    loads = [
        pltpu.make_async_copy(src, dst, load_sem.at[i])
        for i, (src, dst) in enumerate(
            [
                (tokens.at[0], xv),
                (latent_down, ldv),
                (query_down, qdv),
                (cache, kc.at[pl.ds(0, CROWS)]),
                (query_up, qupv),
                (key_up, kupv),
            ]
        )
    ]
    for copy in loads:
        copy.start()

    barrier = pltpu.get_barrier_semaphore()

    def greet(**where):
        pl.semaphore_signal(barrier, inc=1, device_id=where, device_id_type=MESH)

    for d in range(1, NHEAD):
        greet(head=(h + d) % NHEAD)
    greet(ctx=partner)

    @pl.when(z < ZS - 1)
    def _():
        greet(ctx=up)

    @pl.when(z == 0)
    def _():
        greet(ctx=down)

    gives = (1 - role) * ((h % 4) // 3)

    @pl.when(gives == 1)
    def _():
        for p in range(NHEAD):
            greet(role=1, head=p)

    first = offset[0]
    lane = lax.broadcasted_iota(jnp.int32, (1, ROWS), 1)
    place_row = jnp.where(role == 0, first + c * ROWS + lane, bounds[...].reshape(1, ROWS))
    limits = jnp.concatenate([place_row] * HEADS, axis=1)
    square = (ROWS, ROWS)
    eye = lax.broadcasted_iota(jnp.int32, square, 0) == lax.broadcasted_iota(jnp.int32, square, 1)
    place_col = jnp.sum(jnp.where(eye, place_row.astype(F32), 0.0), axis=1, keepdims=True)
    angles = place_col * freqs[...]
    cos[...] = jnp.cos(angles)
    sines = jnp.sin(angles)
    sin[...] = jnp.where(lax.broadcasted_iota(jnp.int32, square, 1) < ROT // 2, -sines, sines)

    with scope("w_x"):
        loads[0].wait()
        loads[1].wait()
    x = xv[...]
    stage_kv[...] = jnp.dot(x, ldv[...], preferred_element_type=F32).astype(BF16)
    loads[2].wait()
    for i in range(QBLOCKS // 2):
        part = jnp.dot(x, qdv[:, 256 * i : 256 * i + 256], preferred_element_type=F32)
        stage_q[2 * i] = part[:, :128]
        stage_q[2 * i + 1] = part[:, 128:]
    loads[3].wait()
    with scope("w_bar"):
        pl.semaphore_wait(barrier, NHEAD + jnp.minimum(z, 1) + z // (ZS - 1) + 4 * role)

    @pl.when(z > 0)
    def _():
        pl.semaphore_signal(ready_z.at[0], inc=1, device_id={"ctx": down}, device_id_type=MESH)

    @pl.when(z == ZS - 1)
    def _():
        pl.semaphore_signal(ready_z.at[1], inc=1, device_id={"ctx": up}, device_id_type=MESH)

    @pl.when(role == 1)
    def _():
        for g in range(4):
            pl.semaphore_signal(
                ready_role.at[0], inc=1, device_id={"role": 0, "head": 4 * g + 3}, device_id_type=MESH
            )

    def cache_rows(s, sub):
        if s == 8:
            s, sub = 0, sub + 1
        return kc.at[pl.ds(s * 4 * CROWS + sub * CROWS, CROWS)]

    def cache_z(s, d):
        return remote(
            cache_rows(s, 0 if s == 0 else d), cache_rows(s + 1, d),
            cz_send.at[8 * d + s], cz_recv.at[8 * d + s], ctx=(up, down)[d],
        )

    def cache_p(s, d):
        return remote(
            cache_rows(s, d), cache_rows(s, 2 + d),
            cp_send.at[9 * d + s], cp_recv.at[9 * d + s], ctx=partner,
        )

    last = (8, 7)

    def start(copy):
        copy.start()
        tail.append(copy)

    def cache_step(s):
        for d in range(2):
            if 0 < s <= last[d]:
                cache_z(s - 1, d).wait_recv()
            if s < last[d]:
                start(cache_z(s, d))
            if s <= last[d] and (s > 0 or d == 0):
                start(cache_p(s, d))

    for d in range(4):
        g = (group + d) % 4
        owner = 4 * g + 3
        copy = remote(
            stage_kv.at[pl.ds(pl.multiple_of(16 * g, 16), 16)], rs_kv.at[h],
            rs_send.at[d], rs_recv.at[h], head=owner,
        )

        @pl.when(owner != h)
        def _():
            copy.start()

        tail.append((owner != h, copy))

    for d in range(QBLOCKS):
        b = (3 * group + jnp.minimum(h % 4, 2) + d) % QBLOCKS
        owner = 4 * (b // 3) + b % 3
        copy = remote(stage_q.at[b], rs_q.at[h], rs_send.at[4 + d], rs_recv.at[h], head=owner)

        @pl.when(owner != h)
        def _():
            copy.start()

        tail.append((owner != h, copy))

    with scope("c0"):

        @pl.when(z < ZS - 1)
        def _():
            pl.semaphore_wait(ready_z.at[0], 1)

        start(cache_z(0, 0))
        start(cache_p(0, 0))

        @pl.when(z > 0)
        def _():
            cache_z(0, 1).start()

    @pl.when(is_kv)
    def _():
        rows = pl.ds(pl.multiple_of(16 * group, 16), 16)
        total = stage_kv[rows, :].astype(F32)
        for d in range(1, NHEAD):
            p = (h + d) % NHEAD
            with scope("w_rskv"):
                remote(rs_kv.at[p], rs_kv.at[p], rs_send.at[0], rs_recv.at[p], head=p).wait_recv()
                total += rs_kv[p].astype(F32)
        lat, rot = total[:, :LAT], total[:, LAT:]
        lat = lat * lax.rsqrt(jnp.mean(lat * lat, axis=-1, keepdims=True) + EPS) * latent_gain[...].reshape(1, LAT)
        rot = rot * cos[rows, :] + swap_halves(rot) * sin[rows, :]
        ks[0, rows, :LAT] = lat.astype(BF16)
        ks[0, rows, LAT:] = rot.astype(BF16)
        mine = ks.at[0, rows]

        for d in range(1, NHEAD):
            remote(
                mine, ks.at[0, rows], kag_send.at[d], kag_recv.at[group], head=(h + d) % NHEAD
            ).start()

    @pl.when(jnp.logical_not(is_kv))
    def _():
        total = stage_q[q_block]
        for d in range(1, NHEAD):
            p = (h + d) % NHEAD
            with scope("w_rsq"):
                remote(rs_q.at[p], rs_q.at[p], rs_send.at[0], rs_recv.at[p], head=p).wait_recv()
                total += rs_q[p]
        qc[q_block] = total
        for d in range(1, NHEAD):
            remote(
                qc.at[q_block], qc.at[q_block], qag_send.at[d], qag_recv.at[q_block],
                head=(h + d) % NHEAD,
            ).start()

    with scope("c12"):

        @pl.when(z == 0)
        def _():
            pl.semaphore_wait(ready_z.at[1], 1)
            cache_z(0, 1).start()

        tail.append(cache_z(0, 1))
        cache_step(1)
        cache_step(2)

    with scope("role"):

        @pl.when(gives == 1)
        def _():
            rows = pl.ds(pl.multiple_of(16 * group, 16), 16)
            pl.semaphore_wait(ready_role.at[0], NHEAD)
            for d in range(NHEAD):
                remote(
                    ks.at[0, rows], ks.at[1, rows], kag_send.at[NHEAD + d], kag_recv.at[4 + group],
                    role=1, head=(h + d) % NHEAD,
                ).start()

    for g in range(4):
        piece = ks.at[0, pl.ds(16 * g, 16)]

        with scope("w_agkv"):

            @pl.when(h != 4 * g + 3)
            def _():
                remote(piece, piece, kag_send.at[0], kag_recv.at[g], head=4 * g + 3).wait_recv()

    @pl.when(role == 1)
    def _():
        for g in range(4):
            piece = ks.at[1, pl.ds(16 * g, 16)]
            with scope("w_agkv1"):
                remote(piece, piece, kag_send.at[0], kag_recv.at[4 + g], role=0, head=4 * g + 3).wait_recv()

    def block_rows(s, sub, k):
        if s == 8:
            s, sub = 0, sub + 1
        return kb.at[s, pl.ds(sub * ROWS + k * PIECE, PIECE)]

    def block_z(s, d, k):
        i = (8 * d + s) * SUBS + k
        src = ks.at[role, pl.ds(k * PIECE, PIECE)] if s == 0 else block_rows(s, d, k)
        return remote(src, block_rows(s + 1, d, k), bz_send.at[i], bz_recv.at[i], ctx=(up, down)[d])

    def block_p(s, d, k):
        i = (9 * d + s) * SUBS + k
        src = ks.at[role, pl.ds(k * PIECE, PIECE)] if s == 0 else block_rows(s, d, k)
        return remote(src, block_rows(s, 2 + d, k), bp_send.at[i], bp_recv.at[i], ctx=partner)

    def block_step(s):
        for k in range(SUBS):
            for d in range(2):
                if 0 < s <= last[d]:
                    block_z(s - 1, d, k).wait_recv()
                if s < last[d]:
                    start(block_z(s, d, k))
                if s <= last[d] and (s > 0 or d == 0):
                    start(block_p(s, d, k))

    block_step(0)
    kb[0, :ROWS] = ks[role]
    for s in range(1, 6):
        with scope(f"bc{s}"):
            block_step(s)
            cache_step(s + 2)

    for b in range(QBLOCKS):
        with scope("w_agq"):

            @pl.when(h != 4 * (b // 3) + b % 3)
            def _():
                remote(qc.at[b], qc.at[b], qag_send.at[0], qag_recv.at[b], head=4 * (b // 3) + b % 3).wait_recv()

    squares = jnp.zeros((ROWS, 128), F32)
    for b in range(QBLOCKS):
        v = qc[b]
        squares += v * v
    inverse = lax.rsqrt(jnp.sum(squares, axis=-1, keepdims=True) * (1.0 / QRANK) + EPS)
    for b in range(QBLOCKS):
        gain = query_gain[pl.ds(128 * b, 128)].reshape(1, 128)
        qn[:, 128 * b : 128 * b + 128] = (qc[b] * inverse * gain).astype(BF16)

    loads[4].wait()
    loads[5].wait()

    def two_heads(i):
        wide = NOPE + ROT
        q = jnp.dot(qn[...], qupv[:, 2 * wide * i : 2 * wide * (i + 1)], preferred_element_type=F32)
        for j in range(2):
            n = 2 * i + j
            rows = slice(ROWS * n, ROWS * (n + 1))
            nope = q[:, wide * j : wide * j + NOPE].astype(BF16)
            rot = q[:, wide * j + NOPE : wide * (j + 1)]
            qs[rows, LAT:] = (rot * cos[...] + swap_halves(rot) * sin[...]).astype(BF16)
            qs[rows, :LAT] = jnp.dot(nope, kupv[n], preferred_element_type=F32).astype(BF16)

    def score_of(keys):
        return SCALE * lax.dot_general(
            keys, qs[...], (((1,), (1,)), ((), ())), preferred_element_type=F32
        )

    def weighted(keys, e):
        return lax.dot_general(
            keys[:, :LAT], e.astype(BF16), (((0,), (0,)), ((), ())), preferred_element_type=F32
        )

    def attend_self():
        keys = ks[0]
        wide = (ROWS, QCOLS)
        own = lax.broadcasted_iota(jnp.int32, wide, 0) == lax.broadcasted_iota(jnp.int32, wide, 1) % ROWS
        m_ref[...] = jnp.sum(jnp.where(own, score_of(keys), 0.0), axis=0, keepdims=True)
        l_ref[...] = jnp.where(lax.broadcasted_iota(jnp.int32, l_ref.shape, 0) == 0, 1.0, 0.0)
        acc[...] = weighted(keys, jnp.where(own, 1.0, 0.0))

    def attend(keys, bases, rows, edge):
        score = score_of(keys)
        row = lax.broadcasted_iota(jnp.int32, (rows, QCOLS), 0)
        score = jnp.concatenate(
            [
                jnp.where(row < edge - base, score[rows * i : rows * (i + 1)], NEG)
                for i, base in enumerate(bases)
            ],
            axis=0,
        )
        old = m_ref[...]
        new = jnp.maximum(old, jnp.max(score, axis=0, keepdims=True))
        fade = jnp.exp(old - new)
        e = jnp.exp(score - new)
        l_ref[...] = l_ref[...] * fade + jnp.sum(e.reshape(-1, 8, QCOLS), axis=0)
        m_ref[...] = new
        acc[...] = acc[...] * fade + weighted(keys, e)

    def place(s, sub):
        if sub % 2 == 0:
            at = z + ZS - s
        else:
            at = z + s + jnp.where(s == 0, ZS // 2, 0)
        return 2 * (at % ZS) + (core if sub < 2 else 1 - core)

    def cache_attend(j):
        bases = [place(2 * j + i // 4, i % 4) * CROWS for i in range(8)]
        keys = kc[pl.ds(pl.multiple_of(j * 8 * CROWS, 16), 8 * CROWS), :]
        attend(keys, bases, CROWS, jnp.minimum(limits, first))

    def block_attend(s):
        attend(kb[s], [first + place(s, i) * ROWS for i in range(4)], ROWS, limits)

    def cache_partner_wait(s):
        for d in range(2):
            if s <= last[d] and (s > 0 or d == 0):
                cache_p(s, d).wait_recv()

    def block_partner_wait(s):
        for d in range(2):
            if s <= last[d] and (s > 0 or d == 0):
                for k in range(SUBS):
                    block_p(s, d, k).wait_recv()

    with scope("h"):
        for i in range(4):
            two_heads(i)
    with scope("b6"):
        block_step(6)
        cache_step(8)
    with scope("self"):
        attend_self()
    with scope("cpw"):
        for s in range(9):
            cache_partner_wait(s)
    with scope("ca01"):

        @pl.loop(0, 2)
        def _(j):
            cache_attend(j)

    with scope("b7"):
        block_step(7)
    with scope("ca23"):

        @pl.loop(2, 4)
        def _(j):
            cache_attend(j)

    with scope("b8"):
        block_step(8)
        for s in range(1, 7):
            block_partner_wait(s)
    with scope("ba16"):

        @pl.loop(1, 7)
        def _(s):
            block_attend(s)

    with scope("bpw"):
        for s in (7, 0, 8):
            block_partner_wait(s)
    with scope("ba78"):

        @pl.loop(7, 9)
        def _(s):
            block_attend(s % 8)

    out[...] = (acc[...] / jnp.sum(l_ref[...], axis=0, keepdims=True)).astype(BF16)

    for item in tail:
        if isinstance(item, tuple):

            @pl.when(item[0])
            def _():
                item[1].wait_send()

        else:
            item.wait_send()

    @pl.when(is_kv)
    def _():
        mine = ks.at[0, pl.ds(pl.multiple_of(16 * group, 16), 16)]
        for d in range(1, NHEAD):
            remote(mine, mine, kag_send.at[d], kag_recv.at[0], head=(h + d) % NHEAD).wait_send()

        @pl.when(role == 0)
        def _():
            for d in range(NHEAD):
                remote(
                    mine, mine, kag_send.at[NHEAD + d], kag_recv.at[0], role=1, head=(h + d) % NHEAD
                ).wait_send()

    @pl.when(jnp.logical_not(is_kv))
    def _():
        for d in range(1, NHEAD):
            remote(
                qc.at[q_block], qc.at[q_block], qag_send.at[d], qag_recv.at[0], head=(h + d) % NHEAD
            ).wait_send()


def values(olat, value_up, out):
    for n in range(HEADS):
        out[:, VAL * n : VAL * (n + 1)] = lax.dot_general(
            olat[:, ROWS * n : ROWS * (n + 1)], value_up[n], (((0,), (0,)), ((), ())),
            preferred_element_type=F32,
        ).astype(BF16)


def local(
    tokens, latent_cache, offset, bounds, query_down, latent_down_weight, query_gain,
    latent_norm_gain, query_up, key_up_transposed, value_up_weight,
):
    freqs = (10000.0 ** (-np.arange(ROT // 2) / (ROT // 2))).astype(np.float32)
    freqs = jnp.asarray(np.concatenate([freqs, freqs])[None, :])

    anywhere = pl.BlockSpec(memory_space=pl.ANY)
    vmem = pl.BlockSpec(memory_space=pltpu.VMEM)
    smem = pl.BlockSpec(memory_space=pltpu.SMEM)
    dma = lambda n: pltpu.SemaphoreType.DMA((n,))
    wide = HEADS * (NOPE + ROT)
    olat = pl.pallas_call(
        body,
        out_shape=jax.ShapeDtypeStruct((LAT, QCOLS), BF16),
        in_specs=[anywhere] * 6 + [smem] + [vmem] * 4,
        out_specs=vmem,
        scratch_shapes=[
            pltpu.VMEM((ROWS, tokens.shape[2]), BF16),
            pltpu.VMEM((tokens.shape[2], KEY), BF16),
            pltpu.VMEM((tokens.shape[2], QRANK), BF16),
            pltpu.VMEM((QRANK, wide), BF16),
            pltpu.VMEM((HEADS, NOPE, LAT), BF16),
            pltpu.VMEM((ROWS, ROT), F32),
            pltpu.VMEM((ROWS, ROT), F32),
            pltpu.VMEM((ROWS, KEY), BF16),
            pltpu.VMEM((QBLOCKS, ROWS, 128), F32),
            pltpu.VMEM((NHEAD, 16, KEY), BF16),
            pltpu.VMEM((NHEAD, ROWS, 128), F32),
            pltpu.VMEM((QBLOCKS, ROWS, 128), F32),
            pltpu.VMEM((2, ROWS, KEY), BF16),
            pltpu.VMEM((NCTX * CROWS, KEY), BF16),
            pltpu.VMEM((8, 4 * ROWS, KEY), BF16),
            pltpu.VMEM((ROWS, QRANK), BF16),
            pltpu.VMEM((QCOLS, KEY), BF16),
            pltpu.VMEM((1, QCOLS), F32),
            pltpu.VMEM((8, QCOLS), F32),
            pltpu.VMEM((LAT, QCOLS), F32),
            dma(6), dma(16), dma(16), dma(16), dma(12), dma(32), dma(8),
            dma(16), dma(16), dma(18), dma(18),
            dma(16 * SUBS), dma(16 * SUBS), dma(18 * SUBS), dma(18 * SUBS),
            pltpu.SemaphoreType.REGULAR((2,)), pltpu.SemaphoreType.REGULAR((1,)),
        ],
        compiler_params=pltpu.CompilerParams(
            collective_id=0, has_side_effects=True, vmem_limit_bytes=56 * 1024 * 1024
        ),
    )(
        tokens, latent_cache, query_down, latent_down_weight, query_up, key_up_transposed,
        offset, bounds, freqs, query_gain, latent_norm_gain,
    )
    result = pl.pallas_call(
        values,
        out_shape=jax.ShapeDtypeStruct((ROWS, HEADS * VAL), BF16),
        in_specs=[vmem, vmem],
        out_specs=vmem,
    )(olat, value_up_weight)
    return result[None]


def solution(mesh):
    return jax.shard_map(
        local,
        mesh=mesh,
        in_specs=(
            P("role", "ctx", "head"),
            P("ctx", None),
            P(),
            P("ctx"),
            P("head", None),
            P("head", None),
            P(),
            P(),
            P(None, "head"),
            P("head", None, None),
            P("head", None, None),
        ),
        out_specs=P("role", "ctx", "head"),
        check_vma=False,
    )
```

```python
import jax
import jax.numpy as jnp
import numpy as np
from jax import lax
from jax.experimental import pallas as pl
from jax.experimental.pallas import tpu as pltpu
from jax.sharding import PartitionSpec as P

LAT = 512
ROT = 64
KEY = LAT + ROT
NOPE = 128
VAL = 128
HEADS = 8
ROWS = 64
CROWS = 48
QRANK = 1536
QBLOCKS = QRANK // 128
ZS = 16
NCTX = 2 * ZS
NHEAD = 16
EPS = 1e-06
SCALE = (NOPE + ROT) ** (-0.5)
NEG = -1e30
MESH = pl.DeviceIdType.MESH
F32 = jnp.float32
BF16 = jnp.bfloat16
SUBS = 2
PIECE = ROWS // SUBS
QCOLS = HEADS * ROWS
scope = jax.named_scope


def remote(src, dst, send, recv, **where):
    return pltpu.make_async_remote_copy(
        src_ref=src, dst_ref=dst, send_sem=send, recv_sem=recv, device_id=where, device_id_type=MESH
    )


def swap_halves(v):
    return jnp.concatenate([v[:, ROT // 2 :], v[:, : ROT // 2]], axis=1)


def body(
    tokens, cache, query_down, latent_down, query_up, key_up, value_up,
    offset, bounds, freqs, query_gain, latent_gain,
    out,
    xv, ldv, qdv, qupv, kupv, vupv, cos, sin,
    stage_kv, stage_q, rs_kv, rs_q, qc, ks, kc, kb, qn, qs, m_ref, l_ref, acc,
    load_sem, rs_send, rs_recv, qag_send, qag_recv, kag_send, kag_recv,
    cz_send, cz_recv, cp_send, cp_recv, bz_send, bz_recv, bp_send, bp_recv,
    ready_z, ready_role,
):
    role = lax.axis_index("role")
    c = lax.axis_index("ctx")
    h = lax.axis_index("head")
    z, core = c // 2, c % 2
    up, down = (c + 2) % NCTX, (c + NCTX - 2) % NCTX
    partner = c + 1 - 2 * core
    group = h // 4
    is_kv = h % 4 == 3
    q_block = 3 * group + h % 4
    tail = []

    loads = [
        pltpu.make_async_copy(src, dst, load_sem.at[i])
        for i, (src, dst) in enumerate(
            [
                (tokens.at[0], xv),
                (latent_down, ldv),
                (query_down, qdv),
                (cache, kc.at[pl.ds(0, CROWS)]),
                (query_up, qupv),
                (key_up, kupv),
                (value_up, vupv),
            ]
        )
    ]
    for copy in loads:
        copy.start()

    barrier = pltpu.get_barrier_semaphore()

    def greet(**where):
        pl.semaphore_signal(barrier, inc=1, device_id=where, device_id_type=MESH)

    for d in range(1, NHEAD):
        greet(head=(h + d) % NHEAD)
    greet(ctx=partner)

    @pl.when(z < ZS - 1)
    def _():
        greet(ctx=up)

    @pl.when(z == 0)
    def _():
        greet(ctx=down)

    gives = (1 - role) * ((h % 4) // 3)

    @pl.when(gives == 1)
    def _():
        for p in range(NHEAD):
            greet(role=1, head=p)

    first = offset[0]
    lane = lax.broadcasted_iota(jnp.int32, (1, ROWS), 1)
    place_row = jnp.where(role == 0, first + c * ROWS + lane, bounds[...].reshape(1, ROWS))
    limits = jnp.concatenate([place_row] * HEADS, axis=1)
    square = (ROWS, ROWS)
    eye = lax.broadcasted_iota(jnp.int32, square, 0) == lax.broadcasted_iota(jnp.int32, square, 1)
    place_col = jnp.sum(jnp.where(eye, place_row.astype(F32), 0.0), axis=1, keepdims=True)
    angles = place_col * freqs[...]
    cos[...] = jnp.cos(angles)
    sines = jnp.sin(angles)
    sin[...] = jnp.where(lax.broadcasted_iota(jnp.int32, square, 1) < ROT // 2, -sines, sines)

    with scope("w_x"):
        loads[0].wait()
        loads[1].wait()
    x = xv[...]
    stage_kv[...] = jnp.dot(x, ldv[...], preferred_element_type=F32).astype(BF16)
    loads[2].wait()
    for i in range(QBLOCKS // 2):
        part = jnp.dot(x, qdv[:, 256 * i : 256 * i + 256], preferred_element_type=F32)
        stage_q[2 * i] = part[:, :128]
        stage_q[2 * i + 1] = part[:, 128:]
    loads[3].wait()
    with scope("w_bar"):
        pl.semaphore_wait(barrier, NHEAD + jnp.minimum(z, 1) + z // (ZS - 1) + 4 * role)

    @pl.when(z > 0)
    def _():
        pl.semaphore_signal(ready_z.at[0], inc=1, device_id={"ctx": down}, device_id_type=MESH)

    @pl.when(z == ZS - 1)
    def _():
        pl.semaphore_signal(ready_z.at[1], inc=1, device_id={"ctx": up}, device_id_type=MESH)

    @pl.when(role == 1)
    def _():
        for g in range(4):
            pl.semaphore_signal(
                ready_role.at[0], inc=1, device_id={"role": 0, "head": 4 * g + 3}, device_id_type=MESH
            )

    def cache_rows(s, sub):
        if s == 8:
            s, sub = 0, sub + 1
        return kc.at[pl.ds(s * 4 * CROWS + sub * CROWS, CROWS)]

    def cache_z(s, d):
        return remote(
            cache_rows(s, 0 if s == 0 else d), cache_rows(s + 1, d),
            cz_send.at[8 * d + s], cz_recv.at[8 * d + s], ctx=(up, down)[d],
        )

    def cache_p(s, d):
        return remote(
            cache_rows(s, d), cache_rows(s, 2 + d),
            cp_send.at[9 * d + s], cp_recv.at[9 * d + s], ctx=partner,
        )

    last = (8, 7)

    def start(copy):
        copy.start()
        tail.append(copy)

    def cache_step(s):
        for d in range(2):
            if 0 < s <= last[d]:
                cache_z(s - 1, d).wait_recv()
            if s < last[d]:
                start(cache_z(s, d))
            if s <= last[d] and (s > 0 or d == 0):
                start(cache_p(s, d))

    for d in range(4):
        g = (group + d) % 4
        owner = 4 * g + 3
        copy = remote(
            stage_kv.at[pl.ds(pl.multiple_of(16 * g, 16), 16)], rs_kv.at[h],
            rs_send.at[d], rs_recv.at[h], head=owner,
        )

        @pl.when(owner != h)
        def _():
            copy.start()

        tail.append((owner != h, copy))

    for d in range(QBLOCKS):
        b = (3 * group + jnp.minimum(h % 4, 2) + d) % QBLOCKS
        owner = 4 * (b // 3) + b % 3
        copy = remote(stage_q.at[b], rs_q.at[h], rs_send.at[4 + d], rs_recv.at[h], head=owner)

        @pl.when(owner != h)
        def _():
            copy.start()

        tail.append((owner != h, copy))

    with scope("c0"):

        @pl.when(z < ZS - 1)
        def _():
            pl.semaphore_wait(ready_z.at[0], 1)

        start(cache_z(0, 0))
        start(cache_p(0, 0))

        @pl.when(z == 0)
        def _():
            pl.semaphore_wait(ready_z.at[1], 1)

        start(cache_z(0, 1))

    for s in range(1, 3):
        with scope(f"c{s}"):
            cache_step(s)

    @pl.when(is_kv)
    def _():
        rows = pl.ds(pl.multiple_of(16 * group, 16), 16)
        total = stage_kv[rows, :].astype(F32)
        for d in range(1, NHEAD):
            p = (h + d) % NHEAD
            with scope("w_rskv"):
                remote(rs_kv.at[p], rs_kv.at[p], rs_send.at[0], rs_recv.at[p], head=p).wait_recv()
                total += rs_kv[p].astype(F32)
        lat, rot = total[:, :LAT], total[:, LAT:]
        lat = lat * lax.rsqrt(jnp.mean(lat * lat, axis=-1, keepdims=True) + EPS) * latent_gain[...].reshape(1, LAT)
        rot = rot * cos[rows, :] + swap_halves(rot) * sin[rows, :]
        ks[0, rows, :LAT] = lat.astype(BF16)
        ks[0, rows, LAT:] = rot.astype(BF16)
        mine = ks.at[0, rows]

        for d in range(1, NHEAD):
            remote(
                mine, ks.at[0, rows], kag_send.at[d], kag_recv.at[group], head=(h + d) % NHEAD
            ).start()

    for s in range(3, 5):
        with scope(f"c{s}"):
            cache_step(s)

    @pl.when(jnp.logical_not(is_kv))
    def _():
        total = stage_q[q_block]
        for d in range(1, NHEAD):
            p = (h + d) % NHEAD
            with scope("w_rsq"):
                remote(rs_q.at[p], rs_q.at[p], rs_send.at[0], rs_recv.at[p], head=p).wait_recv()
                total += rs_q[p]
        qc[q_block] = total
        for d in range(1, NHEAD):
            remote(
                qc.at[q_block], qc.at[q_block], qag_send.at[d], qag_recv.at[q_block],
                head=(h + d) % NHEAD,
            ).start()

    with scope("c5"):
        cache_step(5)

    with scope("role"):

        @pl.when(gives == 1)
        def _():
            rows = pl.ds(pl.multiple_of(16 * group, 16), 16)
            pl.semaphore_wait(ready_role.at[0], NHEAD)
            for d in range(NHEAD):
                remote(
                    ks.at[0, rows], ks.at[1, rows], kag_send.at[NHEAD + d], kag_recv.at[4 + group],
                    role=1, head=(h + d) % NHEAD,
                ).start()

    for g in range(4):
        piece = ks.at[0, pl.ds(16 * g, 16)]

        with scope("w_agkv"):

            @pl.when(h != 4 * g + 3)
            def _():
                remote(piece, piece, kag_send.at[0], kag_recv.at[g], head=4 * g + 3).wait_recv()

    @pl.when(role == 1)
    def _():
        for g in range(4):
            piece = ks.at[1, pl.ds(16 * g, 16)]
            with scope("w_agkv1"):
                remote(piece, piece, kag_send.at[0], kag_recv.at[4 + g], role=0, head=4 * g + 3).wait_recv()

    def block_rows(s, sub, k):
        if s == 8:
            s, sub = 0, sub + 1
        return kb.at[s, pl.ds(sub * ROWS + k * PIECE, PIECE)]

    def block_z(s, d, k):
        i = (8 * d + s) * SUBS + k
        src = ks.at[role, pl.ds(k * PIECE, PIECE)] if s == 0 else block_rows(s, d, k)
        return remote(src, block_rows(s + 1, d, k), bz_send.at[i], bz_recv.at[i], ctx=(up, down)[d])

    def block_p(s, d, k):
        i = (9 * d + s) * SUBS + k
        src = ks.at[role, pl.ds(k * PIECE, PIECE)] if s == 0 else block_rows(s, d, k)
        return remote(src, block_rows(s, 2 + d, k), bp_send.at[i], bp_recv.at[i], ctx=partner)

    def block_step(s):
        for k in range(SUBS):
            for d in range(2):
                if 0 < s <= last[d]:
                    block_z(s - 1, d, k).wait_recv()
                if s < last[d]:
                    start(block_z(s, d, k))
                if s <= last[d] and (s > 0 or d == 0):
                    start(block_p(s, d, k))

    block_step(0)
    kb[0, :ROWS] = ks[role]
    for s in range(1, 4):
        with scope(f"bc{s}"):
            block_step(s)
            cache_step(s + 5)
    with scope("b4"):
        block_step(4)

    for b in range(QBLOCKS):
        with scope("w_agq"):

            @pl.when(h != 4 * (b // 3) + b % 3)
            def _():
                remote(qc.at[b], qc.at[b], qag_send.at[0], qag_recv.at[b], head=4 * (b // 3) + b % 3).wait_recv()

    squares = jnp.zeros((ROWS, 128), F32)
    for b in range(QBLOCKS):
        v = qc[b]
        squares += v * v
    inverse = lax.rsqrt(jnp.sum(squares, axis=-1, keepdims=True) * (1.0 / QRANK) + EPS)
    for b in range(QBLOCKS):
        gain = query_gain[pl.ds(128 * b, 128)].reshape(1, 128)
        qn[:, 128 * b : 128 * b + 128] = (qc[b] * inverse * gain).astype(BF16)

    loads[4].wait()
    loads[5].wait()

    def two_heads(i):
        wide = NOPE + ROT
        q = jnp.dot(qn[...], qupv[:, 2 * wide * i : 2 * wide * (i + 1)], preferred_element_type=F32)
        for j in range(2):
            n = 2 * i + j
            rows = slice(ROWS * n, ROWS * (n + 1))
            nope = q[:, wide * j : wide * j + NOPE].astype(BF16)
            rot = q[:, wide * j + NOPE : wide * (j + 1)]
            qs[rows, LAT:] = (rot * cos[...] + swap_halves(rot) * sin[...]).astype(BF16)
            qs[rows, :LAT] = jnp.dot(nope, kupv[n], preferred_element_type=F32).astype(BF16)

    def score_of(keys):
        return SCALE * lax.dot_general(
            keys, qs[...], (((1,), (1,)), ((), ())), preferred_element_type=F32
        )

    def weighted(keys, e):
        return lax.dot_general(
            keys[:, :LAT], e.astype(BF16), (((0,), (0,)), ((), ())), preferred_element_type=F32
        )

    def attend_self():
        keys = ks[0]
        wide = (ROWS, QCOLS)
        own = lax.broadcasted_iota(jnp.int32, wide, 0) == lax.broadcasted_iota(jnp.int32, wide, 1) % ROWS
        m_ref[...] = jnp.sum(jnp.where(own, score_of(keys), 0.0), axis=0, keepdims=True)
        l_ref[...] = jnp.where(lax.broadcasted_iota(jnp.int32, l_ref.shape, 0) == 0, 1.0, 0.0)
        acc[...] = weighted(keys, jnp.where(own, 1.0, 0.0))

    def attend(keys, bases, rows, edge):
        score = score_of(keys)
        row = lax.broadcasted_iota(jnp.int32, (rows, QCOLS), 0)
        score = jnp.concatenate(
            [
                jnp.where(row < edge - base, score[rows * i : rows * (i + 1)], NEG)
                for i, base in enumerate(bases)
            ],
            axis=0,
        )
        old = m_ref[...]
        new = jnp.maximum(old, jnp.max(score, axis=0, keepdims=True))
        fade = jnp.exp(old - new)
        e = jnp.exp(score - new)
        l_ref[...] = l_ref[...] * fade + jnp.sum(e.reshape(-1, 8, QCOLS), axis=0)
        m_ref[...] = new
        acc[...] = acc[...] * fade + weighted(keys, e)

    def place(s, sub):
        if sub % 2 == 0:
            at = z + ZS - s
        else:
            at = z + s + jnp.where(s == 0, ZS // 2, 0)
        return 2 * (at % ZS) + (core if sub < 2 else 1 - core)

    def cache_attend(j):
        bases = [place(2 * j + i // 4, i % 4) * CROWS for i in range(8)]
        keys = kc[pl.ds(pl.multiple_of(j * 8 * CROWS, 16), 8 * CROWS), :]
        attend(keys, bases, CROWS, jnp.minimum(limits, first))

    def block_attend(s):
        attend(kb[s], [first + place(s, i) * ROWS for i in range(4)], ROWS, limits)

    def cache_partner_wait(s):
        for d in range(2):
            if s <= last[d] and (s > 0 or d == 0):
                cache_p(s, d).wait_recv()

    def block_partner_wait(s):
        for d in range(2):
            if s <= last[d] and (s > 0 or d == 0):
                for k in range(SUBS):
                    block_p(s, d, k).wait_recv()

    def block_attends(low, high):
        with scope(f"ba{low}"):

            @pl.loop(low, high)
            def _(s):
                block_attend(s % 8)

    def cache_attends(low, high):
        with scope(f"ca{low}"):

            @pl.loop(low, high)
            def _(j):
                cache_attend(j)

    with scope("h01"):
        two_heads(0)
        two_heads(1)
    with scope("b5"):
        block_step(5)
    with scope("h23"):
        two_heads(2)
        two_heads(3)
    with scope("b6"):
        block_step(6)
    attend_self()
    with scope("cpw"):
        for s in range(9):
            cache_partner_wait(s)
    cache_attends(0, 2)
    with scope("b7"):
        block_step(7)
    cache_attends(2, 4)
    with scope("bpw1"):
        block_partner_wait(1)
        block_partner_wait(2)
    block_attends(1, 3)
    with scope("b8"):
        block_step(8)
        for s in range(3, 7):
            block_partner_wait(s)
    block_attends(3, 7)
    with scope("bpw"):
        for s in (7, 0, 8):
            block_partner_wait(s)
    block_attends(7, 9)

    loads[6].wait()
    scale = 1.0 / jnp.sum(l_ref[...], axis=0, keepdims=True)
    for n in range(HEADS):
        columns = slice(ROWS * n, ROWS * (n + 1))
        olat = (acc[:, columns] * scale[:, columns]).astype(BF16)
        out[:, VAL * n : VAL * (n + 1)] = lax.dot_general(
            olat, vupv[n], (((0,), (0,)), ((), ())), preferred_element_type=F32
        )

    for item in tail:
        if isinstance(item, tuple):

            @pl.when(item[0])
            def _():
                item[1].wait_send()

        else:
            item.wait_send()

    @pl.when(is_kv)
    def _():
        mine = ks.at[0, pl.ds(pl.multiple_of(16 * group, 16), 16)]
        for d in range(1, NHEAD):
            remote(mine, mine, kag_send.at[d], kag_recv.at[0], head=(h + d) % NHEAD).wait_send()

        @pl.when(role == 0)
        def _():
            for d in range(NHEAD):
                remote(
                    mine, mine, kag_send.at[NHEAD + d], kag_recv.at[0], role=1, head=(h + d) % NHEAD
                ).wait_send()

    @pl.when(jnp.logical_not(is_kv))
    def _():
        for d in range(1, NHEAD):
            remote(
                qc.at[q_block], qc.at[q_block], qag_send.at[d], qag_recv.at[0], head=(h + d) % NHEAD
            ).wait_send()


def local(
    tokens, latent_cache, offset, bounds, query_down, latent_down_weight, query_gain,
    latent_norm_gain, query_up, key_up_transposed, value_up_weight,
):
    freqs = (10000.0 ** (-np.arange(ROT // 2) / (ROT // 2))).astype(np.float32)
    freqs = jnp.asarray(np.concatenate([freqs, freqs])[None, :])

    anywhere = pl.BlockSpec(memory_space=pl.ANY)
    vmem = pl.BlockSpec(memory_space=pltpu.VMEM)
    smem = pl.BlockSpec(memory_space=pltpu.SMEM)
    dma = lambda n: pltpu.SemaphoreType.DMA((n,))
    wide = HEADS * (NOPE + ROT)
    result = pl.pallas_call(
        body,
        out_shape=jax.ShapeDtypeStruct((ROWS, HEADS * VAL), F32),
        in_specs=[anywhere] * 7 + [smem] + [vmem] * 4,
        out_specs=vmem,
        scratch_shapes=[
            pltpu.VMEM((ROWS, tokens.shape[2]), BF16),
            pltpu.VMEM((tokens.shape[2], KEY), BF16),
            pltpu.VMEM((tokens.shape[2], QRANK), BF16),
            pltpu.VMEM((QRANK, wide), BF16),
            pltpu.VMEM((HEADS, NOPE, LAT), BF16),
            pltpu.VMEM((HEADS, LAT, VAL), BF16),
            pltpu.VMEM((ROWS, ROT), F32),
            pltpu.VMEM((ROWS, ROT), F32),
            pltpu.VMEM((ROWS, KEY), BF16),
            pltpu.VMEM((QBLOCKS, ROWS, 128), F32),
            pltpu.VMEM((NHEAD, 16, KEY), BF16),
            pltpu.VMEM((NHEAD, ROWS, 128), F32),
            pltpu.VMEM((QBLOCKS, ROWS, 128), F32),
            pltpu.VMEM((2, ROWS, KEY), BF16),
            pltpu.VMEM((NCTX * CROWS, KEY), BF16),
            pltpu.VMEM((8, 4 * ROWS, KEY), BF16),
            pltpu.VMEM((ROWS, QRANK), BF16),
            pltpu.VMEM((QCOLS, KEY), BF16),
            pltpu.VMEM((1, QCOLS), F32),
            pltpu.VMEM((8, QCOLS), F32),
            pltpu.VMEM((LAT, QCOLS), F32),
            dma(7), dma(16), dma(16), dma(16), dma(12), dma(32), dma(8),
            dma(16), dma(16), dma(18), dma(18),
            dma(16 * SUBS), dma(16 * SUBS), dma(18 * SUBS), dma(18 * SUBS),
            pltpu.SemaphoreType.REGULAR((2,)), pltpu.SemaphoreType.REGULAR((1,)),
        ],
        compiler_params=pltpu.CompilerParams(
            collective_id=0, has_side_effects=True, vmem_limit_bytes=56 * 1024 * 1024
        ),
    )(
        tokens, latent_cache, query_down, latent_down_weight, query_up, key_up_transposed,
        value_up_weight, offset, bounds, freqs, query_gain, latent_norm_gain,
    )
    return result.astype(BF16)[None]


def solution(mesh):
    return jax.shard_map(
        local,
        mesh=mesh,
        in_specs=(
            P("role", "ctx", "head"),
            P("ctx", None),
            P(),
            P("ctx"),
            P("head", None),
            P("head", None),
            P(),
            P(),
            P(None, "head"),
            P("head", None, None),
            P("head", None, None),
        ),
        out_specs=P("role", "ctx", "head"),
        check_vma=False,
    )
```

```python
import jax
import jax.numpy as jnp
import numpy as np
from jax import lax
from jax.experimental import pallas as pl
from jax.experimental.pallas import tpu as pltpu
from jax.sharding import PartitionSpec as P

LAT = 512
ROT = 64
KEY = LAT + ROT
NOPE = 128
VAL = 128
HEADS = 8
ROWS = 64
CROWS = 48
QRANK = 1536
QBLOCKS = QRANK // 128
ZS = 16
NCTX = 2 * ZS
NHEAD = 16
EPS = 1e-06
SCALE = (NOPE + ROT) ** (-0.5)
NEG = -1e30
MESH = pl.DeviceIdType.MESH
F32 = jnp.float32
BF16 = jnp.bfloat16
SUBS = 2
PIECE = ROWS // SUBS
QCOLS = HEADS * ROWS
scope = jax.named_scope


def remote(src, dst, send, recv, **where):
    return pltpu.make_async_remote_copy(
        src_ref=src, dst_ref=dst, send_sem=send, recv_sem=recv, device_id=where, device_id_type=MESH
    )


def swap_halves(v):
    return jnp.concatenate([v[:, ROT // 2 :], v[:, : ROT // 2]], axis=1)


def body(
    tokens, cache, query_down, latent_down, query_up, key_up, value_up,
    offset, bounds, freqs, query_gain, latent_gain,
    out,
    xv, ldv, qdv, qupv, kupv, vupv, cos, sin,
    stage_kv, stage_q, rs_kv, rs_q, qc, ks, kc, kb, qn, qs, m_ref, l_ref, acc,
    load_sem, rs_send, rs_recv, qag_send, qag_recv, kag_send, kag_recv,
    cz_send, cz_recv, cp_send, cp_recv, bz_send, bz_recv, bp_send, bp_recv,
    ready_z, ready_role,
):
    role = lax.axis_index("role")
    c = lax.axis_index("ctx")
    h = lax.axis_index("head")
    z, core = c // 2, c % 2
    up, down = (c + 2) % NCTX, (c + NCTX - 2) % NCTX
    partner = c + 1 - 2 * core
    group = h // 4
    is_kv = h % 4 == 3
    q_block = 3 * group + h % 4
    tail = []

    loads = [
        pltpu.make_async_copy(src, dst, load_sem.at[i])
        for i, (src, dst) in enumerate(
            [
                (tokens.at[0], xv),
                (latent_down, ldv),
                (query_down, qdv),
                (cache, kc.at[pl.ds(0, CROWS)]),
                (query_up, qupv),
                (key_up, kupv),
                (value_up, vupv),
            ]
        )
    ]
    for copy in loads:
        copy.start()

    barrier = pltpu.get_barrier_semaphore()

    def greet(**where):
        pl.semaphore_signal(barrier, inc=1, device_id=where, device_id_type=MESH)

    for d in range(1, NHEAD):
        greet(head=(h + d) % NHEAD)
    greet(ctx=partner)

    @pl.when(z < ZS - 1)
    def _():
        greet(ctx=up)

    @pl.when(z == 0)
    def _():
        greet(ctx=down)

    gives = (1 - role) * ((h % 4) // 3)

    @pl.when(gives == 1)
    def _():
        for p in range(NHEAD):
            greet(role=1, head=p)

    first = offset[0]
    lane = lax.broadcasted_iota(jnp.int32, (1, ROWS), 1)
    place_row = jnp.where(role == 0, first + c * ROWS + lane, bounds[...].reshape(1, ROWS))
    limits = jnp.concatenate([place_row] * HEADS, axis=1)
    square = (ROWS, ROWS)
    eye = lax.broadcasted_iota(jnp.int32, square, 0) == lax.broadcasted_iota(jnp.int32, square, 1)
    place_col = jnp.sum(jnp.where(eye, place_row.astype(F32), 0.0), axis=1, keepdims=True)
    angles = place_col * freqs[...]
    cos[...] = jnp.cos(angles)
    sines = jnp.sin(angles)
    sin[...] = jnp.where(lax.broadcasted_iota(jnp.int32, square, 1) < ROT // 2, -sines, sines)

    with scope("w_x"):
        loads[0].wait()
        loads[1].wait()
    x = xv[...]
    stage_kv[...] = jnp.dot(x, ldv[...], preferred_element_type=F32).astype(BF16)
    loads[2].wait()
    for i in range(QBLOCKS // 2):
        part = jnp.dot(x, qdv[:, 256 * i : 256 * i + 256], preferred_element_type=F32)
        stage_q[2 * i] = part[:, :128]
        stage_q[2 * i + 1] = part[:, 128:]
    loads[3].wait()
    with scope("w_bar"):
        pl.semaphore_wait(barrier, NHEAD + jnp.minimum(z, 1) + z // (ZS - 1) + 4 * role)

    @pl.when(z > 0)
    def _():
        pl.semaphore_signal(ready_z.at[0], inc=1, device_id={"ctx": down}, device_id_type=MESH)

    @pl.when(z == ZS - 1)
    def _():
        pl.semaphore_signal(ready_z.at[1], inc=1, device_id={"ctx": up}, device_id_type=MESH)

    @pl.when(role == 1)
    def _():
        for g in range(4):
            pl.semaphore_signal(
                ready_role.at[0], inc=1, device_id={"role": 0, "head": 4 * g + 3}, device_id_type=MESH
            )

    def cache_rows(s, sub):
        if s == 8:
            s, sub = 0, sub + 1
        return kc.at[pl.ds(s * 4 * CROWS + sub * CROWS, CROWS)]

    def cache_z(s, d):
        return remote(
            cache_rows(s, 0 if s == 0 else d), cache_rows(s + 1, d),
            cz_send.at[8 * d + s], cz_recv.at[8 * d + s], ctx=(up, down)[d],
        )

    def cache_p(s, d):
        return remote(
            cache_rows(s, d), cache_rows(s, 2 + d),
            cp_send.at[9 * d + s], cp_recv.at[9 * d + s], ctx=partner,
        )

    last = (8, 7)

    def start(copy):
        copy.start()
        tail.append(copy)

    def cache_step(s):
        for d in range(2):
            if 0 < s <= last[d]:
                cache_z(s - 1, d).wait_recv()
            if s < last[d]:
                start(cache_z(s, d))
            if s <= last[d] and (s > 0 or d == 0):
                start(cache_p(s, d))

    for d in range(4):
        g = (group + d) % 4
        owner = 4 * g + 3
        copy = remote(
            stage_kv.at[pl.ds(pl.multiple_of(16 * g, 16), 16)], rs_kv.at[h],
            rs_send.at[d], rs_recv.at[h], head=owner,
        )

        @pl.when(owner != h)
        def _():
            copy.start()

        tail.append((owner != h, copy))

    for d in range(QBLOCKS):
        b = (3 * group + jnp.minimum(h % 4, 2) + d) % QBLOCKS
        owner = 4 * (b // 3) + b % 3
        copy = remote(stage_q.at[b], rs_q.at[h], rs_send.at[4 + d], rs_recv.at[h], head=owner)

        @pl.when(owner != h)
        def _():
            copy.start()

        tail.append((owner != h, copy))

    with scope("c0"):

        @pl.when(z < ZS - 1)
        def _():
            pl.semaphore_wait(ready_z.at[0], 1)

        start(cache_z(0, 0))
        start(cache_p(0, 0))

        @pl.when(z == 0)
        def _():
            pl.semaphore_wait(ready_z.at[1], 1)

        start(cache_z(0, 1))

    for s in range(1, 3):
        with scope(f"c{s}"):
            cache_step(s)

    @pl.when(is_kv)
    def _():
        rows = pl.ds(pl.multiple_of(16 * group, 16), 16)
        total = stage_kv[rows, :].astype(F32)
        for d in range(1, NHEAD):
            p = (h + d) % NHEAD
            with scope("w_rskv"):
                remote(rs_kv.at[p], rs_kv.at[p], rs_send.at[0], rs_recv.at[p], head=p).wait_recv()
                total += rs_kv[p].astype(F32)
        lat, rot = total[:, :LAT], total[:, LAT:]
        lat = lat * lax.rsqrt(jnp.mean(lat * lat, axis=-1, keepdims=True) + EPS) * latent_gain[...].reshape(1, LAT)
        rot = rot * cos[rows, :] + swap_halves(rot) * sin[rows, :]
        ks[0, rows, :LAT] = lat.astype(BF16)
        ks[0, rows, LAT:] = rot.astype(BF16)
        mine = ks.at[0, rows]

        for d in range(1, NHEAD):
            remote(
                mine, ks.at[0, rows], kag_send.at[d], kag_recv.at[group], head=(h + d) % NHEAD
            ).start()

    for s in range(3, 5):
        with scope(f"c{s}"):
            cache_step(s)


    with scope("role"):

        @pl.when(gives == 1)
        def _():
            rows = pl.ds(pl.multiple_of(16 * group, 16), 16)
            pl.semaphore_wait(ready_role.at[0], NHEAD)
            for d in range(NHEAD):
                remote(
                    ks.at[0, rows], ks.at[1, rows], kag_send.at[NHEAD + d], kag_recv.at[4 + group],
                    role=1, head=(h + d) % NHEAD,
                ).start()

    for g in range(4):
        piece = ks.at[0, pl.ds(16 * g, 16)]

        with scope("w_agkv"):

            @pl.when(h != 4 * g + 3)
            def _():
                remote(piece, piece, kag_send.at[0], kag_recv.at[g], head=4 * g + 3).wait_recv()

    @pl.when(role == 1)
    def _():
        for g in range(4):
            piece = ks.at[1, pl.ds(16 * g, 16)]
            with scope("w_agkv1"):
                remote(piece, piece, kag_send.at[0], kag_recv.at[4 + g], role=0, head=4 * g + 3).wait_recv()

    def block_rows(s, sub, k):
        if s == 8:
            s, sub = 0, sub + 1
        return kb.at[s, pl.ds(sub * ROWS + k * PIECE, PIECE)]

    def block_z(s, d, k):
        i = (8 * d + s) * SUBS + k
        src = ks.at[role, pl.ds(k * PIECE, PIECE)] if s == 0 else block_rows(s, d, k)
        return remote(src, block_rows(s + 1, d, k), bz_send.at[i], bz_recv.at[i], ctx=(up, down)[d])

    def block_p(s, d, k):
        i = (9 * d + s) * SUBS + k
        src = ks.at[role, pl.ds(k * PIECE, PIECE)] if s == 0 else block_rows(s, d, k)
        return remote(src, block_rows(s, 2 + d, k), bp_send.at[i], bp_recv.at[i], ctx=partner)

    def block_step(s):
        for k in range(SUBS):
            for d in range(2):
                if 0 < s <= last[d]:
                    block_z(s - 1, d, k).wait_recv()
                if s < last[d]:
                    start(block_z(s, d, k))
                if s <= last[d] and (s > 0 or d == 0):
                    start(block_p(s, d, k))

    left = list(tail)
    tail.clear()
    block_step(0)

    @pl.when(jnp.logical_not(is_kv))
    def _():
        total = stage_q[q_block]
        for d in range(1, NHEAD):
            p = (h + d) % NHEAD
            with scope("w_rsq"):
                remote(rs_q.at[p], rs_q.at[p], rs_send.at[0], rs_recv.at[p], head=p).wait_recv()
                total += rs_q[p]
        qc[q_block] = total
        for d in range(1, NHEAD):
            remote(
                qc.at[q_block], qc.at[q_block], qag_send.at[d], qag_recv.at[q_block],
                head=(h + d) % NHEAD,
            ).start()

    kb[0, :ROWS] = ks[role]
    with scope("c5"):
        cache_step(5)
    for s in range(1, 4):
        with scope(f"bc{s}"):
            block_step(s)
            cache_step(s + 5)
    def drain(items):
        for item in items:
            if isinstance(item, tuple):

                @pl.when(item[0])
                def _():
                    item[1].wait_send()

            else:
                item.wait_send()

    drain(left)

    @pl.when(is_kv)
    def _():
        mine = ks.at[0, pl.ds(pl.multiple_of(16 * group, 16), 16)]
        for d in range(1, NHEAD):
            remote(mine, mine, kag_send.at[d], kag_recv.at[0], head=(h + d) % NHEAD).wait_send()

        @pl.when(role == 0)
        def _():
            for d in range(NHEAD):
                remote(
                    mine, mine, kag_send.at[NHEAD + d], kag_recv.at[0], role=1, head=(h + d) % NHEAD
                ).wait_send()

    with scope("b4"):
        block_step(4)

    for b in range(QBLOCKS):
        with scope("w_agq"):

            @pl.when(h != 4 * (b // 3) + b % 3)
            def _():
                remote(qc.at[b], qc.at[b], qag_send.at[0], qag_recv.at[b], head=4 * (b // 3) + b % 3).wait_recv()

    squares = jnp.zeros((ROWS, 128), F32)
    for b in range(QBLOCKS):
        v = qc[b]
        squares += v * v
    inverse = lax.rsqrt(jnp.sum(squares, axis=-1, keepdims=True) * (1.0 / QRANK) + EPS)
    for b in range(QBLOCKS):
        gain = query_gain[pl.ds(128 * b, 128)].reshape(1, 128)
        qn[:, 128 * b : 128 * b + 128] = (qc[b] * inverse * gain).astype(BF16)

    loads[4].wait()
    loads[5].wait()

    def two_heads(i):
        wide = NOPE + ROT
        q = jnp.dot(qn[...], qupv[:, 2 * wide * i : 2 * wide * (i + 1)], preferred_element_type=F32)
        for j in range(2):
            n = 2 * i + j
            rows = slice(ROWS * n, ROWS * (n + 1))
            nope = q[:, wide * j : wide * j + NOPE].astype(BF16)
            rot = q[:, wide * j + NOPE : wide * (j + 1)]
            qs[rows, LAT:] = (rot * cos[...] + swap_halves(rot) * sin[...]).astype(BF16)
            qs[rows, :LAT] = jnp.dot(nope, kupv[n], preferred_element_type=F32).astype(BF16)

    def score_of(keys):
        return SCALE * lax.dot_general(
            keys, qs[...], (((1,), (1,)), ((), ())), preferred_element_type=F32
        )

    def weighted(keys, e):
        return lax.dot_general(
            keys[:, :LAT], e.astype(BF16), (((0,), (0,)), ((), ())), preferred_element_type=F32
        )

    def attend_self():
        keys = ks[0]
        wide = (ROWS, QCOLS)
        own = lax.broadcasted_iota(jnp.int32, wide, 0) == lax.broadcasted_iota(jnp.int32, wide, 1) % ROWS
        m_ref[...] = jnp.sum(jnp.where(own, score_of(keys), 0.0), axis=0, keepdims=True)
        l_ref[...] = jnp.where(lax.broadcasted_iota(jnp.int32, l_ref.shape, 0) == 0, 1.0, 0.0)
        acc[...] = weighted(keys, jnp.where(own, 1.0, 0.0))

    def attend(keys, bases, rows, edge):
        score = score_of(keys)
        row = lax.broadcasted_iota(jnp.int32, (rows, QCOLS), 0)
        score = jnp.concatenate(
            [
                jnp.where(row < edge - base, score[rows * i : rows * (i + 1)], NEG)
                for i, base in enumerate(bases)
            ],
            axis=0,
        )
        old = m_ref[...]
        new = jnp.maximum(old, jnp.max(score, axis=0, keepdims=True))
        fade = jnp.exp(old - new)
        e = jnp.exp(score - new)
        l_ref[...] = l_ref[...] * fade + jnp.sum(e.reshape(-1, 8, QCOLS), axis=0)
        m_ref[...] = new
        acc[...] = acc[...] * fade + weighted(keys, e)

    def place(s, sub):
        if sub % 2 == 0:
            at = z + ZS - s
        else:
            at = z + s + jnp.where(s == 0, ZS // 2, 0)
        return 2 * (at % ZS) + (core if sub < 2 else 1 - core)

    def cache_attend(j):
        bases = [place(2 * j + i // 4, i % 4) * CROWS for i in range(8)]
        keys = kc[pl.ds(pl.multiple_of(j * 8 * CROWS, 16), 8 * CROWS), :]
        attend(keys, bases, CROWS, jnp.minimum(limits, first))

    def block_attend(s):
        attend(kb[s], [first + place(s, i) * ROWS for i in range(4)], ROWS, limits)

    def cache_partner_wait(s):
        for d in range(2):
            if s <= last[d] and (s > 0 or d == 0):
                cache_p(s, d).wait_recv()

    def block_partner_wait(s):
        for d in range(2):
            if s <= last[d] and (s > 0 or d == 0):
                for k in range(SUBS):
                    block_p(s, d, k).wait_recv()

    def block_attends(low, high):
        with scope(f"ba{low}"):

            @pl.loop(low, high)
            def _(s):
                block_attend(s % 8)

    def cache_attends(low, high):
        with scope(f"ca{low}"):

            @pl.loop(low, high)
            def _(j):
                cache_attend(j)

    with scope("h01"):
        two_heads(0)
        two_heads(1)
    with scope("b5"):
        block_step(5)
    with scope("h23"):
        two_heads(2)
        two_heads(3)
    with scope("b6"):
        block_step(6)
    attend_self()
    with scope("cpw"):
        for s in range(9):
            cache_partner_wait(s)
    cache_attends(0, 2)
    with scope("b7"):
        block_step(7)
    cache_attends(2, 4)
    with scope("bpw1"):
        block_partner_wait(1)
        block_partner_wait(2)
    block_attends(1, 3)
    with scope("b8"):
        block_step(8)
        for s in range(3, 7):
            block_partner_wait(s)
    block_attends(3, 7)

    @pl.when(jnp.logical_not(is_kv))
    def _():
        for d in range(1, NHEAD):
            remote(
                qc.at[q_block], qc.at[q_block], qag_send.at[d], qag_recv.at[0], head=(h + d) % NHEAD
            ).wait_send()

    with scope("bpw"):
        for s in (7, 0, 8):
            block_partner_wait(s)
    block_attends(7, 9)

    loads[6].wait()
    scale = 1.0 / jnp.sum(l_ref[...], axis=0, keepdims=True)
    for n in range(HEADS):
        columns = slice(ROWS * n, ROWS * (n + 1))
        olat = (acc[:, columns] * scale[:, columns]).astype(BF16)
        out[:, VAL * n : VAL * (n + 1)] = lax.dot_general(
            olat, vupv[n], (((0,), (0,)), ((), ())), preferred_element_type=F32
        )

    drain(tail)


def local(
    tokens, latent_cache, offset, bounds, query_down, latent_down_weight, query_gain,
    latent_norm_gain, query_up, key_up_transposed, value_up_weight,
):
    freqs = (10000.0 ** (-np.arange(ROT // 2) / (ROT // 2))).astype(np.float32)
    freqs = jnp.asarray(np.concatenate([freqs, freqs])[None, :])

    anywhere = pl.BlockSpec(memory_space=pl.ANY)
    vmem = pl.BlockSpec(memory_space=pltpu.VMEM)
    smem = pl.BlockSpec(memory_space=pltpu.SMEM)
    dma = lambda n: pltpu.SemaphoreType.DMA((n,))
    wide = HEADS * (NOPE + ROT)
    result = pl.pallas_call(
        body,
        out_shape=jax.ShapeDtypeStruct((ROWS, HEADS * VAL), F32),
        in_specs=[anywhere] * 7 + [smem] + [vmem] * 4,
        out_specs=vmem,
        scratch_shapes=[
            pltpu.VMEM((ROWS, tokens.shape[2]), BF16),
            pltpu.VMEM((tokens.shape[2], KEY), BF16),
            pltpu.VMEM((tokens.shape[2], QRANK), BF16),
            pltpu.VMEM((QRANK, wide), BF16),
            pltpu.VMEM((HEADS, NOPE, LAT), BF16),
            pltpu.VMEM((HEADS, LAT, VAL), BF16),
            pltpu.VMEM((ROWS, ROT), F32),
            pltpu.VMEM((ROWS, ROT), F32),
            pltpu.VMEM((ROWS, KEY), BF16),
            pltpu.VMEM((QBLOCKS, ROWS, 128), F32),
            pltpu.VMEM((NHEAD, 16, KEY), BF16),
            pltpu.VMEM((NHEAD, ROWS, 128), F32),
            pltpu.VMEM((QBLOCKS, ROWS, 128), F32),
            pltpu.VMEM((2, ROWS, KEY), BF16),
            pltpu.VMEM((NCTX * CROWS, KEY), BF16),
            pltpu.VMEM((8, 4 * ROWS, KEY), BF16),
            pltpu.VMEM((ROWS, QRANK), BF16),
            pltpu.VMEM((QCOLS, KEY), BF16),
            pltpu.VMEM((1, QCOLS), F32),
            pltpu.VMEM((8, QCOLS), F32),
            pltpu.VMEM((LAT, QCOLS), F32),
            dma(7), dma(16), dma(16), dma(16), dma(12), dma(32), dma(8),
            dma(16), dma(16), dma(18), dma(18),
            dma(16 * SUBS), dma(16 * SUBS), dma(18 * SUBS), dma(18 * SUBS),
            pltpu.SemaphoreType.REGULAR((2,)), pltpu.SemaphoreType.REGULAR((1,)),
        ],
        compiler_params=pltpu.CompilerParams(
            collective_id=0, has_side_effects=True, vmem_limit_bytes=56 * 1024 * 1024
        ),
    )(
        tokens, latent_cache, query_down, latent_down_weight, query_up, key_up_transposed,
        value_up_weight, offset, bounds, freqs, query_gain, latent_norm_gain,
    )
    return result.astype(BF16)[None]


def solution(mesh):
    return jax.shard_map(
        local,
        mesh=mesh,
        in_specs=(
            P("role", "ctx", "head"),
            P("ctx", None),
            P(),
            P("ctx"),
            P("head", None),
            P("head", None),
            P(),
            P(),
            P(None, "head"),
            P("head", None, None),
            P("head", None, None),
        ),
        out_specs=P("role", "ctx", "head"),
        check_vma=False,
    )
```
